256 devices in a mesh: grp: 4 (over y, x), ctx: 32 (over z), hd: 2 (over core).
Axes of the slice: x: 2, y: 2, z: 32, core: 2. Of those that a mesh axis runs over, the one named last changes fastest.
The devices are a block of a 4x8x32 slice.
Arguments:
- queries: bfloat16 [1024, 32, 128], P(('grp', 'ctx'), 'hd'), parts along dimension 0, may hold values from -200 to 200
- prefix_keys: bfloat16 [262144, 4, 128], P(('grp', 'ctx'), 'hd'), parts along dimension 0, may hold values from -6 to 6
- prefix_values: bfloat16 [262144, 4, 128], P(('grp', 'ctx'), 'hd'), parts along dimension 0, may hold values from -6 to 6
- out_weight: bfloat16 [4096, 2048], P(('hd', 'ctx')), may hold values from -0.09375 to 0.09375
- residual_in: bfloat16 [1024, 2048], P(('grp', 'ctx', 'hd')), parts along dimension 0, may hold values from -6 to 6
- expert_ids: int32 [1024, 8], P(('grp', 'ctx', 'hd')), parts along dimension 0, may hold values from 0 to 63, all different within a row; in each aligned block of 4 rows (0 to 3, 4 to 7, ...) at most 2 rows name the same one
- gate_weights: float32 [1024, 8], P(('grp', 'ctx', 'hd')), parts along dimension 0, may hold values from 0.05 to 0.4
- w_gate: bfloat16 [64, 2048, 768], P(('ctx', 'hd')), may hold values from -0.125 to 0.125
- w_up: bfloat16 [64, 2048, 768], P(('ctx', 'hd')), may hold values from -0.125 to 0.125
- w_down: bfloat16 [64, 768, 2048], P(('ctx', 'hd')), may hold values from -0.21875 to 0.21875
Outputs:
- layer_out: bfloat16 [1024, 2048], P(('grp', 'ctx', 'hd')), parts along dimension 0
The draws below stay inside these ranges and needn't reach their ends.
There are 4 independent parts, one for each index of `grp`. The reference program is written for one: setup_inputs(seed, part) draws one part's arguments, and reference() takes and returns one part's arrays. A program takes and returns all parts, laid end to end along the dimension named above; an argument that names none is the same for every part. Nothing has to cross between parts.
Inputs may be any that keep to these rules, and one draw needn't show every extreme that they name: `expert_ids`: each row names 8 different experts; within each aligned block of 4 rows no expert is named by more than 2 rows.
All inputs are finite; a program needn't handle non-finite values.
Results may differ from the reference program's by a relative error of at most 0.013.
Values may be sent and summed in bfloat16 or wider, within the bound.
No kernel may reach another device: no remote copies, remote signals or barrier semaphores. Data moves between devices by JAX's collectives and lax.ppermute only.
A program may use at most 128 MiB of HBM per device.

```python
import math
import jax
import jax.numpy as jnp
import numpy as np
from jax import lax

D = 2048
HEADS = 32
KV_HEADS = 4
HEAD_DIM = 128
FFN = 768
TOP = 8
TOK_DEV = 4
KV_BLOCK = 512
PREFIX = 65536
TOKENS = 256
EXPERTS = 64
CAP = 2


def draw_queries(key, part):
    array_shape = (TOKENS, HEADS, HEAD_DIM)
    standard = jax.random.normal(jax.random.fold_in(key, 11), array_shape, jnp.float32)
    drawn = standard * 2.5
    return jnp.clip(drawn, -200.0, 200.0).astype(jnp.bfloat16)


def shard_levels(rng, extent, cuts, smallest, top_value):
    def one(axis_at, blocks):
        heights = jax.random.uniform(jax.random.fold_in(jax.random.fold_in(rng, 6), axis_at), (blocks,), jnp.float32, smallest / len(cuts), top_value / len(cuts))
        return jnp.repeat(jnp.exp(heights), extent[axis_at] // blocks).reshape((-1,) + (1,) * (len(extent) - axis_at - 1))

    factor_of = one(*cuts[0])
    for cut in cuts[1:]:
        factor_of = factor_of * one(*cut)
    return factor_of


def shared_out(key, own, number, rows, count, top, limit, lean):
    ranking = jax.random.permutation(key, count)
    crowded, usual = load_shares(count, rows * top, limit, lean, True), load_shares(count, rows * top, limit, lean, False)
    places = jnp.arange(count)

    def named(sizes, rotation):
        used = int((sizes > 0).sum())
        fixed = max(1, used // 4)
        shifted = fixed + (places - fixed + rotation * (used - fixed)) % max(1, count - fixed)
        return jnp.zeros((count,), jnp.int32).at[ranking[jnp.where(places < fixed, places, shifted)]].set(jnp.asarray(sizes, jnp.int32))

    sizes = jnp.where(number % 4 == 0, named(crowded, number // 4), named(usual, number - number // 4 - 1))
    mixed = jax.random.permutation(jax.random.fold_in(own, 3), count)
    giver, sink = mixed[0:count // 2 * 2:2], mixed[1:count // 2 * 2:2]
    room = jnp.minimum(sizes[giver] - 1, limit - sizes[sink]) // 2
    room = jnp.where((giver == ranking[0]) | (sink == ranking[0]) | (sizes[sink] == 0), 0, jnp.maximum(room, 0))
    shifted = jax.random.randint(jax.random.fold_in(own, 4), (count // 2,), 0, 1 << 20) % (room + 1)
    sizes = sizes.at[giver].add(-shifted).at[sink].add(shifted)
    items = jnp.searchsorted(jnp.cumsum(sizes), jnp.arange(rows * top), side="right").astype(jnp.int32)
    listing = items.reshape(top, rows).T
    listing = listing[jax.random.permutation(jax.random.fold_in(own, 1), rows)]
    rotation = jax.random.randint(jax.random.fold_in(own, 2), (rows, 1), 0, top)
    return jnp.take_along_axis(listing, (jnp.arange(top)[None, :] + rotation) % top, axis=1)


def load_shares(number_of, total, reach, skew, full):
    loads = [(1 << 20) // math.isqrt(standing ** skew) + 1 for standing in range(1, number_of + 1)]
    largest = reach if full else min(reach, max(-(-total // number_of), total * loads[0] // sum(loads)))
    least = 1 if total - largest >= number_of - 1 else 0
    counts, rest = [largest] + [least] * (number_of - 1), total - largest - least * (number_of - 1)
    while rest > 0:
        candidates = [i for i in range(1, number_of) if counts[i] < largest] or [i for i in range(1, number_of) if counts[i] < reach]
        pool, remaining = sum([loads[i] for i in candidates]), rest
        for i in candidates:
            extra = min(reach - counts[i], max(1, remaining * loads[i] // pool), rest)
            counts[i] = counts[i] + extra
            rest = rest - extra
    return np.array(counts)


def centred(key, shape, scale, most, cuts=(), kind=jnp.bfloat16):
    array = jax.random.normal(key, shape, jnp.float32) * scale
    if len(cuts) > 0:
        array = shard_levels(key, shape, cuts, -0.22, 0.18) * array
    return jnp.clip(array, min=-most, max=most).astype(kind)


def setup_inputs(seed: int = 0, part: int = 0) -> dict:
    keys = jax.random.split(jax.random.key(seed), 11)
    part_keys = jax.random.split(jax.random.fold_in(keys[10], part), 11)
    queries = draw_queries(jax.random.fold_in(jax.random.fold_in(keys[10], part), 71), part)
    prefix_keys = centred(part_keys[1], (PREFIX, KV_HEADS, HEAD_DIM), 1.0, 6.0, ((0, 32), (1, 2)))
    prefix_values = centred(part_keys[2], (PREFIX, KV_HEADS, HEAD_DIM), 1.0, 6.0, ((0, 32), (1, 2)))
    out_weight = centred(keys[3], (HEADS * HEAD_DIM, D), (HEADS * HEAD_DIM) ** -0.5, 0.09375, ((0, 64),))
    residual_in = centred(part_keys[4], (TOKENS, D), 1.0, 6.0, ((0, 64),))
    expert_ids_keys = jax.random.split(jax.random.fold_in(part_keys[5], 1), TOKENS // TOK_DEV)
    expert_ids_turns = jax.random.permutation(jax.random.fold_in(part_keys[5], 3), TOKENS // TOK_DEV)
    expert_ids = jax.vmap(lambda own, number: shared_out(jax.random.fold_in(part_keys[5], 2), own, number, TOK_DEV, EXPERTS, TOP, CAP, 2))(expert_ids_keys, expert_ids_turns).reshape((TOKENS, TOP))
    gate_weights = jnp.clip(jnp.exp(math.log(0.4) - 2.0794415 * jax.random.uniform(part_keys[6], (TOKENS, TOP), jnp.float32) ** shard_levels(part_keys[6], (TOKENS, TOP), ((0, 64),), -0.2, 0.2)), 0.05, 0.4)
    w_gate = centred(keys[7], (EXPERTS, D, FFN), D ** -0.5, 0.125, ((0, 64),))
    w_up = centred(keys[8], (EXPERTS, D, FFN), D ** -0.5, 0.125, ((0, 64),))
    w_down = centred(keys[9], (EXPERTS, FFN, D), FFN ** -0.5, 0.21875, ((0, 64),))
    return dict(queries=queries, prefix_keys=prefix_keys, prefix_values=prefix_values, out_weight=out_weight, residual_in=residual_in, expert_ids=expert_ids, gate_weights=gate_weights, w_gate=w_gate, w_up=w_up, w_down=w_down)


NEG_START = -1e+30

def prefix_attention(queries, prefix_keys, prefix_values):
    grouped = HEADS // KV_HEADS
    query_view = queries.reshape(TOKENS, KV_HEADS, grouped, HEAD_DIM).astype(jnp.float32)
    block_count = PREFIX // KV_BLOCK
    key_blocks = prefix_keys.reshape(block_count, KV_BLOCK, KV_HEADS, HEAD_DIM)
    value_blocks = prefix_values.reshape(block_count, KV_BLOCK, KV_HEADS, HEAD_DIM)
    scaling = HEAD_DIM ** (-0.5)

    def advance(running, pieces):
        peak_scores, totals, accumulated = running
        key_piece, value_piece = pieces
        scores = jnp.einsum('sgjd,kgd->sgjk', query_view, key_piece.astype(jnp.float32)) * scaling
        block_peak = lax.optimization_barrier(jnp.max(scores, axis=-1))
        weights = jnp.exp(scores - block_peak[..., None]).astype(jnp.bfloat16)
        weights = lax.optimization_barrier(weights).astype(jnp.float32)
        block_total = lax.optimization_barrier(jnp.sum(weights, axis=-1))
        block_out = jnp.einsum('sgjk,kgd->sgjd', weights, value_piece.astype(jnp.float32))
        raised = jnp.maximum(peak_scores, block_peak)
        old_factor = jnp.exp(peak_scores - raised)
        new_factor = jnp.exp(block_peak - raised)
        totals = totals * old_factor + block_total * new_factor
        accumulated = accumulated * old_factor[..., None] + block_out * new_factor[..., None]
        return ((raised, totals, accumulated), None)
    start_state = (jnp.full((TOKENS, KV_HEADS, grouped), NEG_START, jnp.float32), jnp.zeros((TOKENS, KV_HEADS, grouped), jnp.float32), jnp.zeros((TOKENS, KV_HEADS, grouped, HEAD_DIM), jnp.float32))
    final_state, leftover = lax.scan(advance, start_state, (key_blocks, value_blocks))
    totals = final_state[1]
    accumulated = final_state[2]
    attended = accumulated / totals[..., None]
    return attended.reshape(TOKENS, HEADS * HEAD_DIM).astype(jnp.bfloat16)

def expert_layer(normed, expert_ids, gate_weights, w_gate, w_up, w_down):
    block_count = TOKENS // TOK_DEV
    slot_total = TOK_DEV * TOP
    id_blocks = expert_ids.reshape(block_count, slot_total)
    expert_iota = jnp.arange(EXPERTS, dtype=jnp.int32)
    onehot = (id_blocks[:, :, None] == expert_iota[None, None, :]).astype(jnp.int32)
    earlier = jnp.cumsum(onehot, axis=1) - onehot
    position = lax.optimization_barrier(jnp.sum(onehot * earlier, axis=2)).astype(jnp.int32)
    slot_iota = jnp.arange(CAP, dtype=jnp.int32)
    dispatch = ((id_blocks[:, None, None, :] == expert_iota[None, :, None, None]) & (position[:, None, None, :] == slot_iota[None, None, :, None])).astype(jnp.float32)
    repeated = jnp.repeat(normed.reshape(block_count, TOK_DEV, D), TOP, axis=1).astype(jnp.float32)
    buffer = jnp.einsum('becn,bnd->ebcd', dispatch, repeated).astype(jnp.bfloat16)

    def run_expert(operands):
        inputs, gate_matrix, up_matrix, down_matrix = operands
        flattened = inputs.reshape(block_count * CAP, D)
        gate_values = jnp.dot(flattened, gate_matrix, preferred_element_type=jnp.float32)
        up_values = jnp.dot(flattened, up_matrix, preferred_element_type=jnp.float32)
        hidden = (jax.nn.silu(gate_values) * up_values).astype(jnp.bfloat16)
        expert_out = jnp.dot(hidden, down_matrix, preferred_element_type=jnp.float32).astype(jnp.bfloat16)
        return expert_out.reshape(block_count, CAP, D)
    results = lax.map(run_expert, (buffer, w_gate, w_up, w_down))
    gathered = jnp.einsum('becn,ebcd->bnd', dispatch, results.astype(jnp.float32))
    weighted = gathered.reshape(TOKENS, TOP, D) * gate_weights[:, :, None]
    return lax.optimization_barrier(jnp.sum(weighted, axis=1))

def reference(queries, prefix_keys, prefix_values, out_weight, residual_in, expert_ids, gate_weights, w_gate, w_up, w_down):
    attended = prefix_attention(queries, prefix_keys, prefix_values)
    projected = jnp.dot(attended, out_weight, preferred_element_type=jnp.float32)
    stream = residual_in.astype(jnp.float32) + projected
    normed = (stream * lax.rsqrt(lax.optimization_barrier(jnp.mean(stream * stream, axis=-1, keepdims=True)) + 1e-06)).astype(jnp.bfloat16)
    mixture = expert_layer(normed, expert_ids, gate_weights, w_gate, w_up, w_down)
    return (stream + mixture).astype(jnp.bfloat16)
```

```python
import math

import jax
import jax.numpy as jnp
from jax import lax
from jax.experimental import pallas as pl
from jax.experimental.pallas import tpu as pltpu
from jax.sharding import PartitionSpec as P

NEAR = 4
BF16 = jnp.bfloat16
F32 = jnp.float32


def contract(a, b, da, db):
    return lax.dot_general(a, b, (((da,), (db,)), ((), ())), preferred_element_type=F32)


def far_groups():
    n = lax.axis_size("ctx")
    return [list(range(r, n, NEAR)) for r in range(NEAR)]


def far_exchange(parts):
    return lax.all_to_all(
        parts, "ctx", split_axis=0, concat_axis=0, axis_index_groups=far_groups(), tiled=True
    )


def far_copies(array):
    members = lax.axis_size("ctx") // NEAR
    return far_exchange(jnp.broadcast_to(array[None], (members, *array.shape)))


def shifted(array, step0, step1):
    n, cores = lax.axis_size("ctx"), lax.axis_size("hd")
    steps = (step0, step1)
    pairs = [
        (i * cores + h, ((i + steps[h % 2]) % n) * cores + h) for i in range(n) for h in range(cores)
    ]
    return lax.ppermute(array, ("ctx", "hd"), pairs)


OFFSET_STEPS = {1: (1, 1), 2: (2, -2), 3: (-1, -1)}


def near_fetch(array, offset):
    a, b = OFFSET_STEPS[offset]
    return shifted(array, -a, -b)


def near_send(array, offset):
    a, b = OFFSET_STEPS[offset]
    return shifted(array, a, b)


def to_partner(array):
    return lax.ppermute(array, "hd", [(0, 1), (1, 0)])


def attention_kernel(c_ref, y0, y1, y2, y3, k_ref, vt_ref, out_ref, qs, vs, st):
    head = pl.program_id(0)
    c = c_ref[0]
    width = k_ref.shape[2]
    rows = qs.shape[0] // NEAR
    half = width // 2
    scale = width ** (-0.5) * math.log2(math.e)
    per_class = st.shape[1] // 4
    group = pl.num_programs(0) // 2

    @pl.when(head % group == 0)
    def _():
        vs[0:width, :] = vt_ref[0]
        vs[width:, :] = jnp.ones((vs.shape[0] - width, vs.shape[1]), BF16)

    for offset, y in enumerate((y0, y1, y2, y3)):
        place = lax.rem(c + offset, NEAR)
        qs[pl.ds(pl.multiple_of(place * rows, rows), rows), :] = (
            y[:, 0].astype(F32).reshape(rows, width)
        )
    q = qs[...].astype(BF16)
    scores = contract(k_ref[0], q, 1, 1)
    peak = jnp.max(scores, axis=0, keepdims=True) * scale
    peak = peak.astype(BF16).astype(F32)
    weights = jnp.exp2(scores * scale - peak).astype(BF16)
    summed = contract(vs[...], weights, 1, 0)
    total = summed[width : width + 1]
    total_hi = total.astype(BF16).astype(F32)

    parity = lax.rem(head, 2)
    row = lax.div(head, 2)
    for p in range(2):
        slot = lax.rem(2 * parity + p - c + NEAR, NEAR)
        out_ref[slot, pl.ds(pl.multiple_of(row * half, half), half), :] = summed[
            p * half : (p + 1) * half
        ].astype(BF16)
    st[parity, pl.ds(row, 1), :] = peak
    st[parity, pl.ds(per_class + row, 1), :] = total_hi
    st[parity, pl.ds(2 * per_class + row, 1), :] = total - total_hi

    @pl.when(head == 0)
    def _():
        st[0, 3 * per_class :, :] = jnp.zeros((per_class, st.shape[2]), F32)
        st[1, 3 * per_class :, :] = jnp.zeros((per_class, st.shape[2]), F32)

    @pl.when(head == pl.num_programs(0) - 1)
    def _():
        for r in range(NEAR):
            slot = lax.rem(r - c + NEAR, NEAR)
            out_ref[slot, per_class * half :, :] = st[r // 2].astype(BF16)


def attention(c, pieces, keys, values_t):
    members, heads, share, width = pieces[0].shape
    tokens = NEAR * members * share
    kv_heads, positions, _ = keys.shape
    group = heads // kv_heads
    per_class = heads // 2
    y_spec = pl.BlockSpec((members, 1, share, width), lambda j, c: (0, j, 0, 0))
    rows_out = per_class * (width // 2) + 4 * per_class
    return pl.pallas_call(
        attention_kernel,
        grid_spec=pltpu.PrefetchScalarGridSpec(
            num_scalar_prefetch=1,
            grid=(heads,),
            in_specs=[
                y_spec,
                y_spec,
                y_spec,
                y_spec,
                pl.BlockSpec((1, positions, width), lambda j, c: (j // group, 0, 0)),
                pl.BlockSpec((1, width, positions), lambda j, c: (j // group, 0, 0)),
            ],
            out_specs=pl.BlockSpec((NEAR, rows_out, tokens), lambda j, c: (0, 0, 0)),
            scratch_shapes=[
                pltpu.VMEM((tokens, width), F32),
                pltpu.VMEM((width + 16, positions), BF16),
                pltpu.VMEM((2, 4 * per_class, tokens), F32),
            ],
        ),
        out_shape=jax.ShapeDtypeStruct((NEAR, rows_out, tokens), BF16),
        compiler_params=pltpu.CompilerParams(dimension_semantics=("arbitrary",)),
        name="attention",
    )(c, *pieces, keys, values_t)


def near_combine_kernel(m0, m1, m2, m3, out_ref):
    count, rows, tokens = out_ref.shape
    half = rows - 8
    sources = (m0, m1, m2, m3)
    stats = [m[count * half :, :].astype(F32) for m in sources]
    peak = stats[0][:count]
    for s in stats[1:]:
        peak = jnp.maximum(peak, s[:count])
    factors = [jnp.exp2(s[:count] - peak) for s in stats]
    total = sum(f * (s[count : 2 * count] + s[2 * count : 3 * count]) for f, s in zip(factors, stats))
    total_hi = total.astype(BF16).astype(F32)
    total_lo = total - total_hi
    place = lax.broadcasted_iota(jnp.int32, (8, tokens), 0)
    for i in range(count):
        acc = sum(
            f[i : i + 1] * m[i * half : (i + 1) * half, :].astype(F32) for f, m in zip(factors, sources)
        )
        out_ref[i, :half, :] = acc.astype(BF16)
        tail = jnp.where(
            place == 0,
            peak[i : i + 1],
            jnp.where(
                place == 1, total_hi[i : i + 1], jnp.where(place == 2, total_lo[i : i + 1], 0.0)
            ),
        )
        out_ref[i, half:, :] = tail.astype(BF16)


def near_combine(sources, count, half):
    tokens = sources[0].shape[1]
    return pl.pallas_call(
        near_combine_kernel,
        out_shape=jax.ShapeDtypeStruct((count, half + 8, tokens), BF16),
        name="near_combine",
    )(*sources)


def project_kernel(where_ref, f_ref, w_ref, own_ref, other_ref):
    members, rows, tokens = f_ref.shape
    half = rows - 8
    c, h = where_ref[0], where_ref[1]
    peaks = [f_ref[i, half:, :].astype(F32) for i in range(members)]
    top = peaks[0][0:1]
    for p in peaks[1:]:
        top = jnp.maximum(top, p[0:1])
    total = jnp.zeros((1, tokens), F32)
    acc = jnp.zeros((half, tokens), F32)
    for i in range(members):
        factor = jnp.exp2(peaks[i][0:1] - top)
        total = total + factor * (peaks[i][1:2] + peaks[i][2:3])
        acc = acc + factor * f_ref[i, :half, :].astype(F32)
    attended = (acc / total).astype(BF16)
    share = tokens // (NEAR * members)
    mine = share // 2
    source = lax.broadcasted_iota(jnp.int32, (tokens, tokens), 0)
    target = lax.broadcasted_iota(jnp.int32, (tokens, tokens), 1)
    side = target // (tokens // 2)
    offset = (target // (members * mine)) % NEAR
    member = (target // mine) % members
    sample = target % mine
    core = (h + side) % 2
    wanted = ((c + offset) % NEAR) * (members * share) + member * share + core * mine + sample
    order = jnp.where(source == wanted, 1.0, 0.0).astype(BF16)
    ordered = contract(attended, order, 1, 0).astype(BF16)
    projected = contract(ordered, w_ref[...], 0, 0)
    own_ref[...] = projected[: tokens // 2]
    other_ref[...] = projected[tokens // 2 :].astype(BF16)


def project(where, arrived, weight):
    tokens = arrived.shape[2]
    model = weight.shape[1]
    return pl.pallas_call(
        project_kernel,
        in_specs=[
            pl.BlockSpec(memory_space=pltpu.SMEM),
            pl.BlockSpec(memory_space=pltpu.VMEM),
            pl.BlockSpec(memory_space=pltpu.VMEM),
        ],
        out_shape=(
            jax.ShapeDtypeStruct((tokens // 2, model), F32),
            jax.ShapeDtypeStruct((tokens // 2, model), BF16),
        ),
        name="project",
    )(where, arrived, weight)


def rows_to_owner(own, other):
    members = lax.axis_size("ctx") // NEAR
    chip = (own.astype(F32) + to_partner(other).astype(F32)).astype(BF16)
    chip = chip.reshape(NEAR, chip.shape[0] // NEAR, chip.shape[1])
    arrived = [near_send(chip[o], o) for o in (1, 2, 3)]
    near = (chip[0].astype(F32) + sum(a.astype(F32) for a in arrived)).astype(BF16)
    far = far_exchange(near.reshape(members, near.shape[0] // members, near.shape[1]))
    return far.astype(F32).sum(axis=0)


def on_device(
    queries,
    prefix_keys,
    prefix_values,
    out_weight,
    residual_in,
    expert_ids,
    gate_weights,
    w_gate,
    w_up,
    w_down,
):
    members = lax.axis_size("ctx") // NEAR
    c = lax.rem(lax.axis_index("ctx"), NEAR).astype(jnp.int32)
    h = lax.axis_index("hd").astype(jnp.int32)
    rows_here, model = residual_in.shape
    experts = lax.axis_size("ctx") * lax.axis_size("hd")

    keys = prefix_keys.transpose(1, 0, 2)
    values_t = prefix_values.transpose(1, 2, 0)
    first = far_copies(queries.transpose(1, 0, 2))
    pieces = [first] + [near_fetch(first, o) for o in (1, 2, 3)]
    partial = attention(c[None], pieces, keys, values_t)
    heads, width = queries.shape[1:]
    arrived = [near_send(partial[o], o) for o in (1, 2, 3)]
    message = near_combine([partial[0], *arrived], heads // 2, width // 2)
    own, other = project(jnp.stack([c, h]), far_exchange(message), out_weight)
    projected = rows_to_owner(own, other)

    stream = residual_in.astype(F32) + projected
    normed = stream * lax.rsqrt(jnp.mean(stream * stream, axis=-1, keepdims=True) + 1e-06)
    named = expert_ids[:, :, None] == jnp.arange(experts, dtype=jnp.int32)[None, None, :]
    coefficient = jnp.sum(jnp.where(named, gate_weights[:, :, None], 0.0), axis=1)
    coefficient_hi = lax.reduce_precision(coefficient, 8, 7)
    message = jnp.concatenate(
        [normed, coefficient_hi, coefficient - coefficient_hi], axis=1
    ).astype(BF16)
    first = far_copies(message).reshape(members * rows_here, model + 2 * experts)
    near = jnp.concatenate([first] + [near_fetch(first, o) for o in (1, 2, 3)], axis=0)
    rows = jnp.concatenate([near, to_partner(near)], axis=0)

    expert = lax.axis_index("ctx") * lax.axis_size("hd") + h
    pick = jnp.arange(2 * experts, dtype=jnp.int32) % experts == expert
    factor = jnp.sum(jnp.where(pick[None], rows[:, model:].astype(F32), 0.0), axis=1, keepdims=True)
    inputs = rows[:, :model]
    gate_values = jnp.dot(inputs, w_gate[0], preferred_element_type=F32)
    up_values = jnp.dot(inputs, w_up[0], preferred_element_type=F32)
    hidden = (jax.nn.silu(gate_values) * up_values).astype(BF16)
    result = jnp.dot(hidden, w_down[0], preferred_element_type=F32)
    weighted = (result * factor).astype(BF16)
    side = weighted.shape[0] // 2
    mixture = rows_to_owner(weighted[:side], weighted[side:])
    return (stream + mixture).astype(BF16)


def solution(mesh):
    placed = (
        P(("grp", "ctx"), "hd", None),
        P(("grp", "ctx"), "hd", None),
        P(("grp", "ctx"), "hd", None),
        P(("hd", "ctx"), None),
        P(("grp", "ctx", "hd"), None),
        P(("grp", "ctx", "hd"), None),
        P(("grp", "ctx", "hd"), None),
        P(("ctx", "hd"), None, None),
        P(("ctx", "hd"), None, None),
        P(("ctx", "hd"), None, None),
    )
    return jax.shard_map(
        on_device,
        mesh=mesh,
        in_specs=placed,
        out_specs=P(("grp", "ctx", "hd"), None),
        check_vma=False,
    )
```

```python
import functools
import math

import jax
import jax.numpy as jnp
from jax import lax
from jax.experimental import pallas as pl
from jax.experimental.pallas import tpu as pltpu
from jax.sharding import PartitionSpec as P

NEAR = 4
BF16 = jnp.bfloat16
F32 = jnp.float32


def contract(a, b, da, db):
    return lax.dot_general(a, b, (((da,), (db,)), ((), ())), preferred_element_type=F32)


def far_groups():
    n = lax.axis_size("ctx")
    return [list(range(r, n, NEAR)) for r in range(NEAR)]


def far_exchange(parts):
    return lax.all_to_all(
        parts, "ctx", split_axis=0, concat_axis=0, axis_index_groups=far_groups(), tiled=True
    )


def far_copies(array):
    members = lax.axis_size("ctx") // NEAR
    return far_exchange(jnp.broadcast_to(array[None], (members, *array.shape)))


def shifted(array, step0, step1):
    n, cores = lax.axis_size("ctx"), lax.axis_size("hd")
    steps = (step0, step1)
    pairs = [
        (i * cores + h, ((i + steps[h % 2]) % n) * cores + h) for i in range(n) for h in range(cores)
    ]
    return lax.ppermute(array, ("ctx", "hd"), pairs)


OFFSET_STEPS = {1: (1, 1), 2: (2, -2), 3: (-1, -1)}


def near_fetch(array, offset):
    a, b = OFFSET_STEPS[offset]
    return shifted(array, -a, -b)


def near_send(array, offset):
    a, b = OFFSET_STEPS[offset]
    return shifted(array, a, b)


def to_partner(array):
    return lax.ppermute(array, "hd", [(0, 1), (1, 0)])


def attention_kernel(
    c_ref, y0, y1, y2, y3, k_ref, vt_ref, out_ref, qs, vs, st, sa, sb, ma, mb, *, kv_head, chunk
):
    c = c_ref[0]
    positions, width = k_ref.shape[1:]
    rows = qs.shape[0] // NEAR
    half = width // 2
    scale = width ** (-0.5) * math.log2(math.e)
    per_class = st.shape[1] // 4
    heads = 2 * per_class
    vs[0:width, :] = vt_ref[kv_head]
    vs[width:, :] = jnp.ones((vs.shape[0] - width, positions), BF16)
    st[...] = jnp.zeros(st.shape, F32)

    def score(head, s_ref, m_ref):
        for offset, y in enumerate((y0, y1, y2, y3)):
            place = lax.rem(c + offset, NEAR)
            qs[pl.ds(pl.multiple_of(place * rows, rows), rows), :] = (
                y[:, kv_head * heads + head].astype(F32).reshape(rows, width)
            )
        q = qs[...].astype(BF16)
        top = None
        for i in range(0, positions, chunk):
            s = contract(k_ref[kv_head, i : i + chunk, :], q, 1, 1)
            s_ref[i : i + chunk, :] = s
            m = jnp.max(s.reshape(chunk // 8, 8, s.shape[1]), axis=0)
            top = m if top is None else jnp.maximum(top, m)
        peak = jnp.max(top, axis=0, keepdims=True) * scale
        m_ref[0:1, :] = peak.astype(BF16).astype(F32)

    def finish(head, s_ref, m_ref):
        peak = m_ref[0:1, :]
        summed = None
        for i in range(0, positions, chunk):
            weights = jnp.exp2(s_ref[i : i + chunk, :] * scale - peak).astype(BF16)
            part = contract(vs[:, i : i + chunk], weights, 1, 0)
            summed = part if summed is None else summed + part
        total = summed[width : width + 1]
        total_hi = total.astype(BF16).astype(F32)
        parity = lax.rem(head, 2)
        row = lax.div(head, 2)
        for p in range(2):
            slot = lax.rem(2 * parity + p - c + NEAR, NEAR)
            out_ref[slot, pl.ds(pl.multiple_of(row * half, half), half), :] = summed[
                p * half : (p + 1) * half
            ].astype(BF16)
        st[parity, pl.ds(row, 1), :] = peak
        st[parity, pl.ds(per_class + row, 1), :] = total_hi
        st[parity, pl.ds(2 * per_class + row, 1), :] = total - total_hi

    score(0, sa, ma)

    def pair(t, carry):
        score(2 * t + 1, sb, mb)
        finish(2 * t, sa, ma)
        score(jnp.minimum(2 * t + 2, heads - 1), sa, ma)
        finish(2 * t + 1, sb, mb)
        return carry

    lax.fori_loop(0, heads // 2, pair, 0)
    for r in range(NEAR):
        slot = lax.rem(r - c + NEAR, NEAR)
        out_ref[slot, per_class * half :, :] = st[r // 2].astype(BF16)


IN_VMEM = pl.BlockSpec(memory_space=pltpu.VMEM)
IN_SMEM = pl.BlockSpec(memory_space=pltpu.SMEM)


def granted(mib):
    return pltpu.CompilerParams(vmem_limit_bytes=mib * 1024 * 1024)


def attention(c, pieces, keys, values_t, kv_head):
    members, all_heads, share, width = pieces[0].shape
    tokens = NEAR * members * share
    kv_heads, positions, _ = keys.shape
    heads = all_heads // kv_heads
    per_class = heads // 2
    rows_out = per_class * (width // 2) + 4 * per_class
    return pl.pallas_call(
        functools.partial(attention_kernel, kv_head=kv_head, chunk=512),
        in_specs=[IN_SMEM] + [IN_VMEM] * 6,
        out_specs=IN_VMEM,
        out_shape=jax.ShapeDtypeStruct((NEAR, rows_out, tokens), BF16),
        scratch_shapes=[
            pltpu.VMEM((tokens, width), F32),
            pltpu.VMEM((width + 16, positions), BF16),
            pltpu.VMEM((2, 4 * per_class, tokens), F32),
            pltpu.VMEM((positions, tokens), F32),
            pltpu.VMEM((positions, tokens), F32),
            pltpu.VMEM((8, tokens), F32),
            pltpu.VMEM((8, tokens), F32),
        ],
        compiler_params=granted(20),
        cost_estimate=pl.CostEstimate(
            flops=4 * heads * tokens * positions * width,
            transcendentals=heads * tokens * positions,
            bytes_accessed=4 * positions * width + 4 * tokens * heads * width,
        ),
        name="attention",
    )(c, *pieces, keys, values_t)


def near_combine_kernel(*refs):
    out_ref = refs[-1]
    count, rows, tokens = out_ref.shape
    half = rows - 8
    place = lax.broadcasted_iota(jnp.int32, (8, tokens), 0)
    sets = (len(refs) - 1) // NEAR
    each = count // sets
    for g in range(sets):
        sources = refs[g * NEAR : (g + 1) * NEAR]
        stats = [m[each * half :, :].astype(F32) for m in sources]
        peak = stats[0][:each]
        for s in stats[1:]:
            peak = jnp.maximum(peak, s[:each])
        factors = [jnp.exp2(s[:each] - peak) for s in stats]
        total = sum(f * (s[each : 2 * each] + s[2 * each : 3 * each]) for f, s in zip(factors, stats))
        total_hi = total.astype(BF16).astype(F32)
        total_lo = total - total_hi
        for i in range(each):
            acc = sum(
                f[i : i + 1] * m[i * half : (i + 1) * half, :].astype(F32)
                for f, m in zip(factors, sources)
            )
            out_ref[g * each + i, :half, :] = acc.astype(BF16)
            tail = jnp.where(
                place == 0,
                peak[i : i + 1],
                jnp.where(
                    place == 1, total_hi[i : i + 1], jnp.where(place == 2, total_lo[i : i + 1], 0.0)
                ),
            )
            out_ref[g * each + i, half:, :] = tail.astype(BF16)


def near_combine(sources, count, half):
    tokens = sources[0].shape[1]
    return pl.pallas_call(
        near_combine_kernel,
        in_specs=[IN_VMEM] * len(sources),
        out_specs=IN_VMEM,
        out_shape=jax.ShapeDtypeStruct((count, half + 8, tokens), BF16),
        compiler_params=granted(12),
        name="near_combine",
    )(*sources)


def project_kernel(where_ref, f_ref, w_ref, own_ref, other_ref):
    members, rows, tokens = f_ref.shape
    half = rows - 8
    c, h = where_ref[0], where_ref[1]
    peaks = [f_ref[i, half:, :].astype(F32) for i in range(members)]
    top = peaks[0][0:1]
    for p in peaks[1:]:
        top = jnp.maximum(top, p[0:1])
    total = jnp.zeros((1, tokens), F32)
    acc = jnp.zeros((half, tokens), F32)
    for i in range(members):
        factor = jnp.exp2(peaks[i][0:1] - top)
        total = total + factor * (peaks[i][1:2] + peaks[i][2:3])
        acc = acc + factor * f_ref[i, :half, :].astype(F32)
    attended = (acc / total).astype(BF16)
    share = tokens // (NEAR * members)
    mine = share // 2
    source = lax.broadcasted_iota(jnp.int32, (tokens, tokens), 0)
    target = lax.broadcasted_iota(jnp.int32, (1, tokens), 1)
    side = target // (tokens // 2)
    offset = (target // (members * mine)) % NEAR
    member = (target // mine) % members
    sample = target % mine
    core = (h + side) % 2
    wanted = ((c + offset) % NEAR) * (members * share) + member * share + core * mine + sample
    order = jnp.where(source == wanted, 1.0, 0.0).astype(BF16)
    ordered = contract(attended, order, 1, 0).astype(BF16)
    projected = contract(ordered, w_ref[...], 0, 0)
    own_ref[...] = projected[: tokens // 2].astype(BF16)
    other_ref[...] = projected[tokens // 2 :].astype(BF16)


def project(where, arrived, weight):
    tokens = arrived.shape[2]
    model = weight.shape[1]
    return pl.pallas_call(
        project_kernel,
        in_specs=[IN_SMEM, IN_VMEM, IN_VMEM],
        out_specs=(IN_VMEM, IN_VMEM),
        out_shape=(
            jax.ShapeDtypeStruct((tokens // 2, model), BF16),
            jax.ShapeDtypeStruct((tokens // 2, model), BF16),
        ),
        compiler_params=granted(12),
        name="project",
    )(where, arrived, weight)


def experts_kernel(e_ref, near_ref, far_ref, g_ref, u_ref, d_ref, own_ref, other_ref, xs, acc):
    step = pl.program_id(0)
    side, wide = near_ref.shape
    model = g_ref.shape[1]

    @pl.when(step == 0)
    def _():
        xs[:side] = near_ref[:, :model]
        xs[side:] = far_ref[:, :model]

    x = xs[...]
    gate = contract(x, g_ref[0], 1, 0)
    up = contract(x, u_ref[0], 1, 0)
    hidden = (gate / (1.0 + jnp.exp(-gate)) * up).astype(BF16)
    part = contract(hidden, d_ref[0], 1, 0)

    @pl.when(step == 0)
    def _():
        acc[...] = part

    @pl.when(step > 0)
    def _():
        acc[...] += part

    @pl.when(step == pl.num_programs(0) - 1)
    def _():
        lane = lax.broadcasted_iota(jnp.int32, (1, wide - model), 1)
        pick = jnp.where(lane % ((wide - model) // 2) == e_ref[0], 1.0, 0.0)
        for rows_ref, out_ref, at in ((near_ref, own_ref, 0), (far_ref, other_ref, side)):
            factor = jnp.sum(rows_ref[:, model:].astype(F32) * pick, axis=1, keepdims=True)
            out_ref[...] = (acc[at : at + side] * factor).astype(BF16)


def run_expert(expert, near, far, w_gate, w_up, w_down):
    side, wide = near.shape
    _, model, ffn = w_gate.shape
    block = 128
    whole = pl.BlockSpec((side, wide), lambda i: (0, 0))
    out = pl.BlockSpec((side, model), lambda i: (0, 0))
    return pl.pallas_call(
        experts_kernel,
        grid=(ffn // block,),
        in_specs=[
            IN_SMEM,
            whole,
            whole,
            pl.BlockSpec((1, model, block), lambda i: (0, 0, i)),
            pl.BlockSpec((1, model, block), lambda i: (0, 0, i)),
            pl.BlockSpec((1, block, model), lambda i: (0, i, 0)),
        ],
        out_specs=(out, out),
        out_shape=(
            jax.ShapeDtypeStruct((side, model), BF16),
            jax.ShapeDtypeStruct((side, model), BF16),
        ),
        scratch_shapes=[pltpu.VMEM((2 * side, model), BF16), pltpu.VMEM((2 * side, model), F32)],
        compiler_params=granted(50),
        name="experts",
    )(expert, near, far, w_gate, w_up, w_down)


def rows_to_owner(own, other):
    members = lax.axis_size("ctx") // NEAR
    chip = (own.astype(F32) + to_partner(other).astype(F32)).astype(BF16)
    chip = chip.reshape(NEAR, chip.shape[0] // NEAR, chip.shape[1])
    arrived = [near_send(chip[o], o) for o in (1, 2, 3)]
    near = (chip[0].astype(F32) + sum(a.astype(F32) for a in arrived)).astype(BF16)
    far = far_exchange(near.reshape(members, near.shape[0] // members, near.shape[1]))
    return far.astype(F32).sum(axis=0)


def on_device(
    queries,
    prefix_keys,
    prefix_values,
    out_weight,
    residual_in,
    expert_ids,
    gate_weights,
    w_gate,
    w_up,
    w_down,
):
    members = lax.axis_size("ctx") // NEAR
    c = lax.rem(lax.axis_index("ctx"), NEAR).astype(jnp.int32)
    h = lax.axis_index("hd").astype(jnp.int32)
    rows_here, model = residual_in.shape
    experts = lax.axis_size("ctx") * lax.axis_size("hd")

    keys = prefix_keys.transpose(1, 0, 2)
    values_t = prefix_values.transpose(1, 2, 0)
    first = far_copies(queries.transpose(1, 0, 2))
    first, keys, values_t = lax.optimization_barrier((first, keys, values_t))
    pieces = [first] + [near_fetch(first, o) for o in (1, 2, 3)]
    heads, width = queries.shape[1:]
    sources = []
    for kv_head in range(keys.shape[0]):
        partial = attention(c[None], pieces, keys, values_t, kv_head)
        sources += [partial[0]] + [near_send(partial[o], o) for o in (1, 2, 3)]
    message = near_combine(sources, heads // 2, width // 2)
    own, other = project(jnp.stack([c, h]), far_exchange(message), out_weight)
    projected = rows_to_owner(own, other)

    stream = residual_in.astype(F32) + projected
    normed = stream * lax.rsqrt(jnp.mean(stream * stream, axis=-1, keepdims=True) + 1e-06)
    named = expert_ids[:, :, None] == jnp.arange(experts, dtype=jnp.int32)[None, None, :]
    coefficient = jnp.sum(jnp.where(named, gate_weights[:, :, None], 0.0), axis=1)
    coefficient_hi = lax.reduce_precision(coefficient, 8, 7)
    message = jnp.concatenate(
        [normed, coefficient_hi, coefficient - coefficient_hi], axis=1
    ).astype(BF16)
    first = far_copies(message).reshape(members * rows_here, model + 2 * experts)
    near = jnp.concatenate([first] + [near_fetch(first, o) for o in (1, 2, 3)], axis=0)
    expert = lax.axis_index("ctx").astype(jnp.int32) * lax.axis_size("hd") + h
    own, other = run_expert(expert[None], near, to_partner(near), w_gate, w_up, w_down)
    mixture = rows_to_owner(own, other)
    return (stream + mixture).astype(BF16)


def solution(mesh):
    placed = (
        P(("grp", "ctx"), "hd", None),
        P(("grp", "ctx"), "hd", None),
        P(("grp", "ctx"), "hd", None),
        P(("hd", "ctx"), None),
        P(("grp", "ctx", "hd"), None),
        P(("grp", "ctx", "hd"), None),
        P(("grp", "ctx", "hd"), None),
        P(("ctx", "hd"), None, None),
        P(("ctx", "hd"), None, None),
        P(("ctx", "hd"), None, None),
    )
    return jax.shard_map(
        on_device,
        mesh=mesh,
        in_specs=placed,
        out_specs=P(("grp", "ctx", "hd"), None),
        check_vma=False,
    )
```

```python
import functools
import math

import jax
import jax.numpy as jnp
from jax import lax
from jax.experimental import pallas as pl
from jax.experimental.pallas import tpu as pltpu
from jax.sharding import PartitionSpec as P

NEAR = 4
BF16 = jnp.bfloat16
F32 = jnp.float32


def contract(a, b, da, db):
    return lax.dot_general(a, b, (((da,), (db,)), ((), ())), preferred_element_type=F32)


def far_groups():
    n = lax.axis_size("ctx")
    return [list(range(r, n, NEAR)) for r in range(NEAR)]


def far_exchange(parts):
    return lax.all_to_all(
        parts, "ctx", split_axis=0, concat_axis=0, axis_index_groups=far_groups(), tiled=True
    )


def far_copies(array):
    members = lax.axis_size("ctx") // NEAR
    return far_exchange(jnp.broadcast_to(array[None], (members, *array.shape)))


def shifted(array, step0, step1):
    n, cores = lax.axis_size("ctx"), lax.axis_size("hd")
    steps = (step0, step1)
    pairs = [
        (i * cores + h, ((i + steps[h % 2]) % n) * cores + h) for i in range(n) for h in range(cores)
    ]
    return lax.ppermute(array, ("ctx", "hd"), pairs)


OFFSET_STEPS = {1: (1, 1), 2: (2, -2), 3: (-1, -1)}
START_ORDER = (2, 1, 3)


def near_fetch(array, offset):
    a, b = OFFSET_STEPS[offset]
    return shifted(array, -a, -b)


def near_fetches(array):
    got = {o: near_fetch(array, o) for o in START_ORDER}
    return [got[o] for o in sorted(got)]


def near_send(array, offset):
    a, b = OFFSET_STEPS[offset]
    return shifted(array, a, b)


def to_partner(array):
    return lax.ppermute(array, "hd", [(0, 1), (1, 0)])


def attention_kernel(
    c_ref, y0, y1, y2, y3, k_ref, vt_ref, out_ref, qs, vs, st, sa, sb, ma, mb, *, kv_head, chunk
):
    c = c_ref[0]
    positions, width = k_ref.shape[1:]
    rows = qs.shape[0] // NEAR
    half = width // 2
    scale = width ** (-0.5) * math.log2(math.e)
    per_class = st.shape[1] // 4
    heads = 2 * per_class
    vs[0:width, :] = vt_ref[kv_head]
    vs[width:, :] = jnp.ones((vs.shape[0] - width, positions), BF16)
    st[...] = jnp.zeros(st.shape, F32)

    def queries_of(head):
        for offset, y in enumerate((y0, y1, y2, y3)):
            place = lax.rem(c + offset, NEAR)
            qs[pl.ds(pl.multiple_of(place * rows, rows), rows), :] = (
                y[:, kv_head * heads + head].astype(F32).reshape(rows, width)
            )
        return qs[...].astype(BF16)

    def advance(head, s_ref, m_ref, next_head, next_s_ref, next_m_ref):
        q = queries_of(next_head)
        peak = None if head is None else m_ref[0:1, :]
        top = summed = None
        for i in range(0, positions, chunk):
            s = contract(k_ref[kv_head, i : i + chunk, :], q, 1, 1)
            next_s_ref[i : i + chunk, :] = s
            m = jnp.max(s.reshape(chunk // 8, 8, s.shape[1]), axis=0)
            top = m if top is None else jnp.maximum(top, m)
            if head is not None:
                weights = jnp.exp2(s_ref[i : i + chunk, :] * scale - peak).astype(BF16)
                part = contract(vs[:, i : i + chunk], weights, 1, 0)
                summed = part if summed is None else summed + part
        next_peak = jnp.max(top, axis=0, keepdims=True) * scale
        next_m_ref[0:1, :] = next_peak.astype(BF16).astype(F32)
        if head is None:
            return
        total = summed[width : width + 1]
        total_hi = total.astype(BF16).astype(F32)
        parity = lax.rem(head, 2)
        row = lax.div(head, 2)
        for p in range(2):
            slot = lax.rem(2 * parity + p - c + NEAR, NEAR)
            out_ref[slot, pl.ds(pl.multiple_of(row * half, half), half), :] = summed[
                p * half : (p + 1) * half
            ].astype(BF16)
        st[parity, pl.ds(row, 1), :] = peak
        st[parity, pl.ds(per_class + row, 1), :] = total_hi
        st[parity, pl.ds(2 * per_class + row, 1), :] = total - total_hi

    advance(None, None, None, 0, sa, ma)

    def pair(t, carry):
        advance(2 * t, sa, ma, 2 * t + 1, sb, mb)
        advance(2 * t + 1, sb, mb, jnp.minimum(2 * t + 2, heads - 1), sa, ma)
        return carry

    lax.fori_loop(0, heads // 2, pair, 0)
    for r in range(NEAR):
        slot = lax.rem(r - c + NEAR, NEAR)
        out_ref[slot, per_class * half :, :] = st[r // 2].astype(BF16)


IN_VMEM = pl.BlockSpec(memory_space=pltpu.VMEM)
IN_SMEM = pl.BlockSpec(memory_space=pltpu.SMEM)


def granted(mib):
    return pltpu.CompilerParams(vmem_limit_bytes=mib * 1024 * 1024)


def attention(c, pieces, keys, values_t, kv_head):
    members, all_heads, share, width = pieces[0].shape
    tokens = NEAR * members * share
    kv_heads, positions, _ = keys.shape
    heads = all_heads // kv_heads
    per_class = heads // 2
    rows_out = per_class * (width // 2) + 4 * per_class
    return pl.pallas_call(
        functools.partial(attention_kernel, kv_head=kv_head, chunk=512),
        in_specs=[IN_SMEM] + [IN_VMEM] * 6,
        out_specs=IN_VMEM,
        out_shape=jax.ShapeDtypeStruct((NEAR, rows_out, tokens), BF16),
        scratch_shapes=[
            pltpu.VMEM((tokens, width), F32),
            pltpu.VMEM((width + 16, positions), BF16),
            pltpu.VMEM((2, 4 * per_class, tokens), F32),
            pltpu.VMEM((positions, tokens), F32),
            pltpu.VMEM((positions, tokens), F32),
            pltpu.VMEM((8, tokens), F32),
            pltpu.VMEM((8, tokens), F32),
        ],
        compiler_params=granted(20),
        cost_estimate=pl.CostEstimate(
            flops=4 * heads * tokens * positions * width,
            transcendentals=heads * tokens * positions,
            bytes_accessed=4 * positions * width + 4 * tokens * heads * width,
        ),
        name="attention",
    )(c, *pieces, keys, values_t)


def near_combine_kernel(*refs):
    out_ref = refs[-1]
    count, rows, tokens = out_ref.shape
    half = rows - 8
    place = lax.broadcasted_iota(jnp.int32, (8, tokens), 0)
    sets = (len(refs) - 1) // NEAR
    each = count // sets
    for g in range(sets):
        sources = refs[g * NEAR : (g + 1) * NEAR]
        stats = [m[each * half :, :].astype(F32) for m in sources]
        peak = stats[0][:each]
        for s in stats[1:]:
            peak = jnp.maximum(peak, s[:each])
        factors = [jnp.exp2(s[:each] - peak) for s in stats]
        total = sum(f * (s[each : 2 * each] + s[2 * each : 3 * each]) for f, s in zip(factors, stats))
        total_hi = total.astype(BF16).astype(F32)
        total_lo = total - total_hi
        for i in range(each):
            acc = sum(
                f[i : i + 1] * m[i * half : (i + 1) * half, :].astype(F32)
                for f, m in zip(factors, sources)
            )
            out_ref[g * each + i, :half, :] = acc.astype(BF16)
            tail = jnp.where(
                place == 0,
                peak[i : i + 1],
                jnp.where(
                    place == 1, total_hi[i : i + 1], jnp.where(place == 2, total_lo[i : i + 1], 0.0)
                ),
            )
            out_ref[g * each + i, half:, :] = tail.astype(BF16)


def near_combine(sources, count, half):
    tokens = sources[0].shape[1]
    return pl.pallas_call(
        near_combine_kernel,
        in_specs=[IN_VMEM] * len(sources),
        out_specs=IN_VMEM,
        out_shape=jax.ShapeDtypeStruct((count, half + 8, tokens), BF16),
        compiler_params=granted(12),
        name="near_combine",
    )(*sources)


def project_kernel(where_ref, f_ref, w_ref, own_ref, other_ref):
    members, rows, tokens = f_ref.shape
    half = rows - 8
    c, h = where_ref[0], where_ref[1]
    peaks = [f_ref[i, half:, :].astype(F32) for i in range(members)]
    top = peaks[0][0:1]
    for p in peaks[1:]:
        top = jnp.maximum(top, p[0:1])
    total = jnp.zeros((1, tokens), F32)
    acc = jnp.zeros((half, tokens), F32)
    for i in range(members):
        factor = jnp.exp2(peaks[i][0:1] - top)
        total = total + factor * (peaks[i][1:2] + peaks[i][2:3])
        acc = acc + factor * f_ref[i, :half, :].astype(F32)
    attended = (acc / total).astype(BF16)
    share = tokens // (NEAR * members)
    mine = share // 2
    source = lax.broadcasted_iota(jnp.int32, (tokens, tokens), 0)
    target = lax.broadcasted_iota(jnp.int32, (1, tokens), 1)
    side = target // (tokens // 2)
    offset = (target // (members * mine)) % NEAR
    member = (target // mine) % members
    sample = target % mine
    core = (h + side) % 2
    wanted = ((c + offset) % NEAR) * (members * share) + member * share + core * mine + sample
    order = jnp.where(source == wanted, 1.0, 0.0).astype(BF16)
    ordered = contract(attended, order, 1, 0).astype(BF16)
    projected = contract(ordered, w_ref[...], 0, 0)
    own_ref[...] = projected[: tokens // 2].astype(BF16)
    other_ref[...] = projected[tokens // 2 :].astype(BF16)


def project(where, arrived, weight):
    tokens = arrived.shape[2]
    model = weight.shape[1]
    return pl.pallas_call(
        project_kernel,
        in_specs=[IN_SMEM, IN_VMEM, IN_VMEM],
        out_specs=(IN_VMEM, IN_VMEM),
        out_shape=(
            jax.ShapeDtypeStruct((tokens // 2, model), BF16),
            jax.ShapeDtypeStruct((tokens // 2, model), BF16),
        ),
        compiler_params=granted(12),
        name="project",
    )(where, arrived, weight)


def experts_kernel(
    e_ref, near_ref, far_ref, g_hbm, u_hbm, d_hbm, own_ref, other_ref, gs, us, ds, xs, hs, sems, *, block, out_block
):
    side, wide = near_ref.shape
    _, model, ffn = g_hbm.shape
    first = [pl.ds(i, block) for i in range(0, ffn, block)]
    second = [pl.ds(i, out_block) for i in range(0, model, out_block)]
    gates = [pltpu.make_async_copy(g_hbm.at[0, :, b], gs.at[:, b], sems.at[0, i]) for i, b in enumerate(first)]
    ups = [pltpu.make_async_copy(u_hbm.at[0, :, b], us.at[:, b], sems.at[1, i]) for i, b in enumerate(first)]
    downs = [pltpu.make_async_copy(d_hbm.at[0, :, b], ds.at[:, b], sems.at[2, i]) for i, b in enumerate(second)]
    for g, u in zip(gates, ups):
        g.start()
        u.start()
    for d in downs:
        d.start()
    xs[:side] = near_ref[:, :model]
    xs[side:] = far_ref[:, :model]
    lane = lax.broadcasted_iota(jnp.int32, (1, wide - model), 1)
    pick = jnp.where(lane % ((wide - model) // 2) == e_ref[0], 1.0, 0.0)
    factors = [
        jnp.sum(r[:, model:].astype(F32) * pick, axis=1, keepdims=True) for r in (near_ref, far_ref)
    ]
    for b, g, u in zip(first, gates, ups):
        g.wait()
        u.wait()
        gate = contract(xs[...], gs[:, b], 1, 0)
        up = contract(xs[...], us[:, b], 1, 0)
        hs[:, b] = (gate / (1.0 + jnp.exp(-gate)) * up).astype(BF16)
    for b, d in zip(second, downs):
        d.wait()
        part = contract(hs[...], ds[:, b], 1, 0)
        own_ref[:, b] = (part[:side] * factors[0]).astype(BF16)
        other_ref[:, b] = (part[side:] * factors[1]).astype(BF16)


def run_expert(expert, near, far, w_gate, w_up, w_down, block=256, out_block=1024, mib=50):
    side, wide = near.shape
    _, model, ffn = w_gate.shape
    in_hbm = pl.BlockSpec(memory_space=pltpu.HBM)
    shape = jax.ShapeDtypeStruct((side, model), BF16)
    return pl.pallas_call(
        functools.partial(experts_kernel, block=block, out_block=out_block),
        in_specs=[IN_SMEM, IN_VMEM, IN_VMEM, in_hbm, in_hbm, in_hbm],
        out_specs=(IN_VMEM, IN_VMEM),
        out_shape=(shape, shape),
        scratch_shapes=[
            pltpu.VMEM((model, ffn), BF16),
            pltpu.VMEM((model, ffn), BF16),
            pltpu.VMEM((ffn, model), BF16),
            pltpu.VMEM((2 * side, model), BF16),
            pltpu.VMEM((2 * side, ffn), BF16),
            pltpu.SemaphoreType.DMA((3, max(ffn // block, model // out_block))),
        ],
        compiler_params=granted(mib),
        name="experts",
    )(expert, near, far, w_gate, w_up, w_down)


def rows_to_owner(own, other):
    members = lax.axis_size("ctx") // NEAR
    chip = (own.astype(F32) + to_partner(other).astype(F32)).astype(BF16)
    chip = chip.reshape(NEAR, chip.shape[0] // NEAR, chip.shape[1])
    arrived = [near_send(chip[o], o) for o in START_ORDER]
    near = (chip[0].astype(F32) + sum(a.astype(F32) for a in arrived)).astype(BF16)
    far = far_exchange(near.reshape(members, near.shape[0] // members, near.shape[1]))
    return far.astype(F32).sum(axis=0)


def on_device(
    queries,
    prefix_keys,
    prefix_values,
    out_weight,
    residual_in,
    expert_ids,
    gate_weights,
    w_gate,
    w_up,
    w_down,
):
    members = lax.axis_size("ctx") // NEAR
    c = lax.rem(lax.axis_index("ctx"), NEAR).astype(jnp.int32)
    h = lax.axis_index("hd").astype(jnp.int32)
    rows_here, model = residual_in.shape
    experts = lax.axis_size("ctx") * lax.axis_size("hd")

    keys = prefix_keys.transpose(1, 0, 2)
    values_t = prefix_values.transpose(1, 2, 0)
    first = far_copies(queries.transpose(1, 0, 2))
    first, keys, values_t = lax.optimization_barrier((first, keys, values_t))
    pieces = [first] + near_fetches(first)
    heads, width = queries.shape[1:]
    sources = []
    for kv_head in range(keys.shape[0]):
        partial = attention(c[None], pieces, keys, values_t, kv_head)
        sources += [partial[0]] + [near_send(partial[o], o) for o in START_ORDER]
    message = near_combine(sources, heads // 2, width // 2)
    own, other = project(jnp.stack([c, h]), far_exchange(message), out_weight)
    projected = rows_to_owner(own, other)

    stream = residual_in.astype(F32) + projected
    normed = stream * lax.rsqrt(jnp.mean(stream * stream, axis=-1, keepdims=True) + 1e-06)
    named = expert_ids[:, :, None] == jnp.arange(experts, dtype=jnp.int32)[None, None, :]
    coefficient = jnp.sum(jnp.where(named, gate_weights[:, :, None], 0.0), axis=1)
    coefficient_hi = lax.reduce_precision(coefficient, 8, 7)
    message = jnp.concatenate(
        [normed, coefficient_hi, coefficient - coefficient_hi], axis=1
    ).astype(BF16)
    first = far_copies(message).reshape(members * rows_here, model + 2 * experts)
    near = jnp.concatenate([first] + near_fetches(first), axis=0)
    expert = lax.axis_index("ctx").astype(jnp.int32) * lax.axis_size("hd") + h
    own, other = run_expert(expert[None], near, to_partner(near), w_gate, w_up, w_down)
    mixture = rows_to_owner(own, other)
    return (stream + mixture).astype(BF16)


def solution(mesh):
    placed = (
        P(("grp", "ctx"), "hd", None),
        P(("grp", "ctx"), "hd", None),
        P(("grp", "ctx"), "hd", None),
        P(("hd", "ctx"), None),
        P(("grp", "ctx", "hd"), None),
        P(("grp", "ctx", "hd"), None),
        P(("grp", "ctx", "hd"), None),
        P(("ctx", "hd"), None, None),
        P(("ctx", "hd"), None, None),
        P(("ctx", "hd"), None, None),
    )
    return jax.shard_map(
        on_device,
        mesh=mesh,
        in_specs=placed,
        out_specs=P(("grp", "ctx", "hd"), None),
        check_vma=False,
    )
```

```python
import functools
import math

import jax
import jax.numpy as jnp
from jax import lax
from jax.experimental import pallas as pl
from jax.experimental.pallas import tpu as pltpu
from jax.sharding import PartitionSpec as P

NEAR = 4
BF16 = jnp.bfloat16
F32 = jnp.float32


def contract(a, b, da, db):
    return lax.dot_general(a, b, (((da,), (db,)), ((), ())), preferred_element_type=F32)


def far_groups():
    n = lax.axis_size("ctx")
    return [list(range(r, n, NEAR)) for r in range(NEAR)]


def far_exchange(parts):
    return lax.all_to_all(
        parts, "ctx", split_axis=0, concat_axis=0, axis_index_groups=far_groups(), tiled=True
    )


def far_copies(array):
    members = lax.axis_size("ctx") // NEAR
    return far_exchange(jnp.broadcast_to(array[None], (members, *array.shape)))


def shifted(array, step0, step1):
    n, cores = lax.axis_size("ctx"), lax.axis_size("hd")
    steps = (step0, step1)
    pairs = [
        (i * cores + h, ((i + steps[h % 2]) % n) * cores + h) for i in range(n) for h in range(cores)
    ]
    return lax.ppermute(array, ("ctx", "hd"), pairs)


OFFSET_STEPS = {1: (1, 1), 2: (2, -2), 3: (-1, -1)}
START_ORDER = (2, 1, 3)


def near_fetch(array, offset):
    a, b = OFFSET_STEPS[offset]
    return shifted(array, -a, -b)


def near_fetches(array):
    got = {o: near_fetch(array, o) for o in START_ORDER}
    return [got[o] for o in sorted(got)]


def near_send(array, offset):
    a, b = OFFSET_STEPS[offset]
    return shifted(array, a, b)


def to_partner(array):
    return lax.ppermute(array, "hd", [(0, 1), (1, 0)])


def attention_kernel(
    c_ref, y0, y1, y2, y3, k_ref, vt_ref, out_ref, qs, vs, st, sa, sb, ma, mb, *, kv_head, chunk
):
    c = c_ref[0]
    positions, width = k_ref.shape[1:]
    rows = qs.shape[0] // NEAR
    half = width // 2
    scale = width ** (-0.5) * math.log2(math.e)
    per_class = st.shape[1] // 4
    heads = 2 * per_class
    vs[0:width, :] = vt_ref[kv_head]
    vs[width:, :] = jnp.ones((vs.shape[0] - width, positions), BF16)
    st[...] = jnp.zeros(st.shape, F32)

    def queries_of(head):
        for offset, y in enumerate((y0, y1, y2, y3)):
            place = lax.rem(c + offset, NEAR)
            qs[pl.ds(pl.multiple_of(place * rows, rows), rows), :] = (
                y[:, head].astype(F32).reshape(rows, width)
            )
        return qs[...].astype(BF16)

    def advance(head, s_ref, m_ref, next_head, next_s_ref, next_m_ref):
        q = queries_of(next_head)
        peak = None if head is None else m_ref[0:1, :]
        top = summed = None
        for i in range(0, positions, chunk):
            s = contract(k_ref[kv_head, i : i + chunk, :], q, 1, 1)
            next_s_ref[i : i + chunk, :] = s
            m = jnp.max(s.reshape(chunk // 8, 8, s.shape[1]), axis=0)
            top = m if top is None else jnp.maximum(top, m)
            if head is not None:
                weights = jnp.exp2(s_ref[i : i + chunk, :] * scale - peak).astype(BF16)
                part = contract(vs[:, i : i + chunk], weights, 1, 0)
                summed = part if summed is None else summed + part
        next_peak = jnp.max(top, axis=0, keepdims=True) * scale
        next_m_ref[0:1, :] = next_peak.astype(BF16).astype(F32)
        if head is None:
            return
        total = summed[width : width + 1]
        total_hi = total.astype(BF16).astype(F32)
        parity = lax.rem(head, 2)
        row = lax.div(head, 2)
        for p in range(2):
            slot = lax.rem(2 * parity + p - c + NEAR, NEAR)
            out_ref[slot, pl.ds(pl.multiple_of(row * half, half), half), :] = summed[
                p * half : (p + 1) * half
            ].astype(BF16)
        st[parity, pl.ds(row, 1), :] = peak
        st[parity, pl.ds(per_class + row, 1), :] = total_hi
        st[parity, pl.ds(2 * per_class + row, 1), :] = total - total_hi

    advance(None, None, None, 0, sa, ma)

    def pair(t, carry):
        advance(2 * t, sa, ma, 2 * t + 1, sb, mb)
        advance(2 * t + 1, sb, mb, jnp.minimum(2 * t + 2, heads - 1), sa, ma)
        return carry

    lax.fori_loop(0, heads // 2, pair, 0)
    for r in range(NEAR):
        slot = lax.rem(r - c + NEAR, NEAR)
        out_ref[slot, per_class * half :, :] = st[r // 2].astype(BF16)


IN_VMEM = pl.BlockSpec(memory_space=pltpu.VMEM)
IN_SMEM = pl.BlockSpec(memory_space=pltpu.SMEM)


def granted(mib):
    return pltpu.CompilerParams(vmem_limit_bytes=mib * 1024 * 1024)


def attention(c, pieces, keys, values_t, kv_head):
    members, heads, share, width = pieces[0].shape
    tokens = NEAR * members * share
    positions = keys.shape[1]
    per_class = heads // 2
    rows_out = per_class * (width // 2) + 4 * per_class
    return pl.pallas_call(
        functools.partial(attention_kernel, kv_head=kv_head, chunk=512),
        in_specs=[IN_SMEM] + [IN_VMEM] * 6,
        out_specs=IN_VMEM,
        out_shape=jax.ShapeDtypeStruct((NEAR, rows_out, tokens), BF16),
        scratch_shapes=[
            pltpu.VMEM((tokens, width), F32),
            pltpu.VMEM((width + 16, positions), BF16),
            pltpu.VMEM((2, 4 * per_class, tokens), F32),
            pltpu.VMEM((positions, tokens), F32),
            pltpu.VMEM((positions, tokens), F32),
            pltpu.VMEM((8, tokens), F32),
            pltpu.VMEM((8, tokens), F32),
        ],
        compiler_params=granted(20),
        cost_estimate=pl.CostEstimate(
            flops=4 * heads * tokens * positions * width,
            transcendentals=heads * tokens * positions,
            bytes_accessed=4 * positions * width + 4 * tokens * heads * width,
        ),
        name="attention",
    )(c, *pieces, keys, values_t)


def near_combine_kernel(*refs):
    out_ref = refs[-1]
    count, rows, tokens = out_ref.shape
    half = rows - 8
    place = lax.broadcasted_iota(jnp.int32, (8, tokens), 0)
    sets = (len(refs) - 1) // NEAR
    each = count // sets
    for g in range(sets):
        sources = refs[g * NEAR : (g + 1) * NEAR]
        stats = [m[each * half :, :].astype(F32) for m in sources]
        peak = stats[0][:each]
        for s in stats[1:]:
            peak = jnp.maximum(peak, s[:each])
        factors = [jnp.exp2(s[:each] - peak) for s in stats]
        total = sum(f * (s[each : 2 * each] + s[2 * each : 3 * each]) for f, s in zip(factors, stats))
        total_hi = total.astype(BF16).astype(F32)
        total_lo = total - total_hi
        for i in range(each):
            acc = sum(
                f[i : i + 1] * m[i * half : (i + 1) * half, :].astype(F32)
                for f, m in zip(factors, sources)
            )
            out_ref[g * each + i, :half, :] = acc.astype(BF16)
            tail = jnp.where(
                place == 0,
                peak[i : i + 1],
                jnp.where(
                    place == 1, total_hi[i : i + 1], jnp.where(place == 2, total_lo[i : i + 1], 0.0)
                ),
            )
            out_ref[g * each + i, half:, :] = tail.astype(BF16)


def near_combine(sources, count, half):
    tokens = sources[0].shape[1]
    return pl.pallas_call(
        near_combine_kernel,
        in_specs=[IN_VMEM] * len(sources),
        out_specs=IN_VMEM,
        out_shape=jax.ShapeDtypeStruct((count, half + 8, tokens), BF16),
        compiler_params=granted(12),
        name="near_combine",
    )(*sources)


def project_kernel(where_ref, f_ref, w_ref, own_ref, other_ref):
    members, rows, tokens = f_ref.shape
    half = rows - 8
    c, h = where_ref[0], where_ref[1]
    peaks = [f_ref[i, half:, :].astype(F32) for i in range(members)]
    top = peaks[0][0:1]
    for p in peaks[1:]:
        top = jnp.maximum(top, p[0:1])
    total = jnp.zeros((1, tokens), F32)
    acc = jnp.zeros((half, tokens), F32)
    for i in range(members):
        factor = jnp.exp2(peaks[i][0:1] - top)
        total = total + factor * (peaks[i][1:2] + peaks[i][2:3])
        acc = acc + factor * f_ref[i, :half, :].astype(F32)
    attended = (acc / total).astype(BF16)
    share = tokens // (NEAR * members)
    mine = share // 2
    source = lax.broadcasted_iota(jnp.int32, (tokens, tokens), 0)
    target = lax.broadcasted_iota(jnp.int32, (1, tokens), 1)
    side = target // (tokens // 2)
    offset = (target // (members * mine)) % NEAR
    member = (target // mine) % members
    sample = target % mine
    core = (h + side) % 2
    wanted = ((c + offset) % NEAR) * (members * share) + member * share + core * mine + sample
    order = jnp.where(source == wanted, 1.0, 0.0).astype(BF16)
    ordered = contract(attended, order, 1, 0).astype(BF16)
    projected = contract(ordered, w_ref[...], 0, 0)
    own_ref[...] = projected[: tokens // 2].astype(BF16)
    other_ref[...] = projected[tokens // 2 :].astype(BF16)


def project(where, arrived, weight):
    tokens = arrived.shape[2]
    model = weight.shape[1]
    return pl.pallas_call(
        project_kernel,
        in_specs=[IN_SMEM, IN_VMEM, IN_VMEM],
        out_specs=(IN_VMEM, IN_VMEM),
        out_shape=(
            jax.ShapeDtypeStruct((tokens // 2, model), BF16),
            jax.ShapeDtypeStruct((tokens // 2, model), BF16),
        ),
        compiler_params=granted(12),
        name="project",
    )(where, arrived, weight)


def experts_kernel(
    e_ref, near_ref, far_ref, g_hbm, u_hbm, d_hbm, own_ref, other_ref, gs, us, ds, xs, hs, sems, *, block, out_block
):
    side, wide = near_ref.shape
    _, model, ffn = g_hbm.shape
    first = [pl.ds(i, block) for i in range(0, ffn, block)]
    second = [pl.ds(i, out_block) for i in range(0, model, out_block)]
    gates = [pltpu.make_async_copy(g_hbm.at[0, :, b], gs.at[:, b], sems.at[0, i]) for i, b in enumerate(first)]
    ups = [pltpu.make_async_copy(u_hbm.at[0, :, b], us.at[:, b], sems.at[1, i]) for i, b in enumerate(first)]
    downs = [pltpu.make_async_copy(d_hbm.at[0, :, b], ds.at[:, b], sems.at[2, i]) for i, b in enumerate(second)]
    for g, u in zip(gates, ups):
        g.start()
        u.start()
    for d in downs:
        d.start()
    xs[:side] = near_ref[:, :model]
    xs[side:] = far_ref[:, :model]
    lane = lax.broadcasted_iota(jnp.int32, (1, wide - model), 1)
    pick = jnp.where(lane % ((wide - model) // 2) == e_ref[0], 1.0, 0.0)
    factors = [
        jnp.sum(r[:, model:].astype(F32) * pick, axis=1, keepdims=True) for r in (near_ref, far_ref)
    ]
    for b, g, u in zip(first, gates, ups):
        g.wait()
        u.wait()
        gate = contract(xs[...], gs[:, b], 1, 0)
        up = contract(xs[...], us[:, b], 1, 0)
        hs[:, b] = (gate / (1.0 + jnp.exp(-gate)) * up).astype(BF16)
    for b, d in zip(second, downs):
        d.wait()
        part = contract(hs[...], ds[:, b], 1, 0)
        own_ref[:, b] = (part[:side] * factors[0]).astype(BF16)
        other_ref[:, b] = (part[side:] * factors[1]).astype(BF16)


def run_expert(expert, near, far, w_gate, w_up, w_down, block=256, out_block=1024, mib=50):
    side, wide = near.shape
    _, model, ffn = w_gate.shape
    in_hbm = pl.BlockSpec(memory_space=pltpu.HBM)
    shape = jax.ShapeDtypeStruct((side, model), BF16)
    return pl.pallas_call(
        functools.partial(experts_kernel, block=block, out_block=out_block),
        in_specs=[IN_SMEM, IN_VMEM, IN_VMEM, in_hbm, in_hbm, in_hbm],
        out_specs=(IN_VMEM, IN_VMEM),
        out_shape=(shape, shape),
        scratch_shapes=[
            pltpu.VMEM((model, ffn), BF16),
            pltpu.VMEM((model, ffn), BF16),
            pltpu.VMEM((ffn, model), BF16),
            pltpu.VMEM((2 * side, model), BF16),
            pltpu.VMEM((2 * side, ffn), BF16),
            pltpu.SemaphoreType.DMA((3, max(ffn // block, model // out_block))),
        ],
        compiler_params=granted(mib),
        name="experts",
    )(expert, near, far, w_gate, w_up, w_down)


def rows_to_owner(own, other):
    members = lax.axis_size("ctx") // NEAR
    chip = (own.astype(F32) + to_partner(other).astype(F32)).astype(BF16)
    chip = chip.reshape(NEAR, chip.shape[0] // NEAR, chip.shape[1])
    arrived = [near_send(chip[o], o) for o in START_ORDER]
    near = (chip[0].astype(F32) + sum(a.astype(F32) for a in arrived)).astype(BF16)
    far = far_exchange(near.reshape(members, near.shape[0] // members, near.shape[1]))
    return far.astype(F32).sum(axis=0)


def on_device(
    queries,
    prefix_keys,
    prefix_values,
    out_weight,
    residual_in,
    expert_ids,
    gate_weights,
    w_gate,
    w_up,
    w_down,
):
    members = lax.axis_size("ctx") // NEAR
    c = lax.rem(lax.axis_index("ctx"), NEAR).astype(jnp.int32)
    h = lax.axis_index("hd").astype(jnp.int32)
    rows_here, model = residual_in.shape
    experts = lax.axis_size("ctx") * lax.axis_size("hd")

    keys = prefix_keys.transpose(1, 0, 2)
    values_t = prefix_values.transpose(1, 2, 0)
    first = far_copies(queries.transpose(1, 0, 2))
    first, keys, values_t = lax.optimization_barrier((first, keys, values_t))
    heads, width = queries.shape[1:]
    kv_heads = keys.shape[0]
    pieces = [[part] + near_fetches(part) for part in jnp.split(first, kv_heads, axis=1)]
    sources = []
    for kv_head in range(kv_heads):
        partial = attention(c[None], pieces[kv_head], keys, values_t, kv_head)
        sources += [partial[0]] + [near_send(partial[o], o) for o in START_ORDER]
    message = near_combine(sources, heads // 2, width // 2)
    own, other = project(jnp.stack([c, h]), far_exchange(message), out_weight)
    projected = rows_to_owner(own, other)

    stream = residual_in.astype(F32) + projected
    normed = stream * lax.rsqrt(jnp.mean(stream * stream, axis=-1, keepdims=True) + 1e-06)
    named = expert_ids[:, :, None] == jnp.arange(experts, dtype=jnp.int32)[None, None, :]
    coefficient = jnp.sum(jnp.where(named, gate_weights[:, :, None], 0.0), axis=1)
    coefficient_hi = lax.reduce_precision(coefficient, 8, 7)
    message = jnp.concatenate(
        [normed, coefficient_hi, coefficient - coefficient_hi], axis=1
    ).astype(BF16)
    first = far_copies(message).reshape(members * rows_here, model + 2 * experts)
    near = jnp.concatenate([first] + near_fetches(first), axis=0)
    expert = lax.axis_index("ctx").astype(jnp.int32) * lax.axis_size("hd") + h
    own, other = run_expert(expert[None], near, to_partner(near), w_gate, w_up, w_down)
    mixture = rows_to_owner(own, other)
    return (stream + mixture).astype(BF16)


def solution(mesh):
    placed = (
        P(("grp", "ctx"), "hd", None),
        P(("grp", "ctx"), "hd", None),
        P(("grp", "ctx"), "hd", None),
        P(("hd", "ctx"), None),
        P(("grp", "ctx", "hd"), None),
        P(("grp", "ctx", "hd"), None),
        P(("grp", "ctx", "hd"), None),
        P(("ctx", "hd"), None, None),
        P(("ctx", "hd"), None, None),
        P(("ctx", "hd"), None, None),
    )
    return jax.shard_map(
        on_device,
        mesh=mesh,
        in_specs=placed,
        out_specs=P(("grp", "ctx", "hd"), None),
        check_vma=False,
    )
```

```python
import functools
import math

import jax
import jax.numpy as jnp
from jax import lax
from jax.experimental import pallas as pl
from jax.experimental.pallas import tpu as pltpu
from jax.sharding import PartitionSpec as P

NEAR = 4
BF16 = jnp.bfloat16
F32 = jnp.float32


def contract(a, b, da, db):
    return lax.dot_general(a, b, (((da,), (db,)), ((), ())), preferred_element_type=F32)


def far_groups():
    n = lax.axis_size("ctx")
    return [list(range(r, n, NEAR)) for r in range(NEAR)]


def far_exchange(parts):
    return lax.all_to_all(
        parts, "ctx", split_axis=0, concat_axis=0, axis_index_groups=far_groups(), tiled=True
    )


def far_copies(array):
    members = lax.axis_size("ctx") // NEAR
    return far_exchange(jnp.broadcast_to(array[None], (members, *array.shape)))


def shifted(array, step0, step1):
    n, cores = lax.axis_size("ctx"), lax.axis_size("hd")
    steps = (step0, step1)
    pairs = [
        (i * cores + h, ((i + steps[h % 2]) % n) * cores + h) for i in range(n) for h in range(cores)
    ]
    return lax.ppermute(array, ("ctx", "hd"), pairs)


OFFSET_STEPS = {1: (1, 1), 2: (2, -2), 3: (-1, -1)}
START_ORDER = (2, 1, 3)


def near_fetch(array, offset):
    a, b = OFFSET_STEPS[offset]
    return shifted(array, -a, -b)


def near_fetches(array):
    return [near_fetch(array, o) for o in START_ORDER]


def near_send(array, offset):
    a, b = OFFSET_STEPS[offset]
    return shifted(array, a, b)


def to_partner(array):
    return lax.ppermute(array, "hd", [(0, 1), (1, 0)])


def attention_kernel(
    c_ref, y0, y1, y2, y3, k_ref, vt_ref, out_ref, qs, vs, st, sa, sb, ma, mb, *, kv_head, chunk
):
    c = c_ref[0]
    positions, width = k_ref.shape[1:]
    rows = qs.shape[0] // NEAR
    half = width // 2
    scale = width ** (-0.5) * math.log2(math.e)
    per_class = st.shape[1] // 4
    heads = 2 * per_class
    vs[0:width, :] = vt_ref[kv_head]
    vs[width:, :] = jnp.ones((vs.shape[0] - width, positions), BF16)
    st[...] = jnp.zeros(st.shape, F32)

    def queries_of(head):
        for offset, y in zip((0, *START_ORDER), (y0, y1, y2, y3)):
            place = lax.rem(c + offset, NEAR)
            qs[pl.ds(pl.multiple_of(place * rows, rows), rows), :] = (
                y[:, head].astype(F32).reshape(rows, width)
            )
        return qs[...].astype(BF16)

    def advance(head, s_ref, m_ref, next_head, next_s_ref, next_m_ref):
        q = queries_of(next_head)
        peak = None if head is None else m_ref[0:1, :]
        top = summed = None
        for i in range(0, positions, chunk):
            s = contract(k_ref[kv_head, i : i + chunk, :], q, 1, 1)
            next_s_ref[i : i + chunk, :] = s
            m = jnp.max(s.reshape(chunk // 8, 8, s.shape[1]), axis=0)
            top = m if top is None else jnp.maximum(top, m)
            if head is not None:
                weights = jnp.exp2(s_ref[i : i + chunk, :] * scale - peak).astype(BF16)
                part = contract(vs[:, i : i + chunk], weights, 1, 0)
                summed = part if summed is None else summed + part
        next_peak = jnp.max(top, axis=0, keepdims=True) * scale
        next_m_ref[0:1, :] = next_peak.astype(BF16).astype(F32)
        if head is None:
            return
        total = summed[width : width + 1]
        total_hi = total.astype(BF16).astype(F32)
        parity = lax.rem(head, 2)
        row = lax.div(head, 2)
        for p in range(2):
            slot = lax.rem(2 * parity + p - c + NEAR, NEAR)
            out_ref[slot, pl.ds(pl.multiple_of(row * half, half), half), :] = summed[
                p * half : (p + 1) * half
            ].astype(BF16)
        st[parity, pl.ds(row, 1), :] = peak
        st[parity, pl.ds(per_class + row, 1), :] = total_hi
        st[parity, pl.ds(2 * per_class + row, 1), :] = total - total_hi

    advance(None, None, None, 0, sa, ma)

    def pair(t, carry):
        advance(2 * t, sa, ma, 2 * t + 1, sb, mb)
        advance(2 * t + 1, sb, mb, jnp.minimum(2 * t + 2, heads - 1), sa, ma)
        return carry

    lax.fori_loop(0, heads // 2, pair, 0)
    for r in range(NEAR):
        slot = lax.rem(r - c + NEAR, NEAR)
        out_ref[slot, per_class * half :, :] = st[r // 2].astype(BF16)


IN_VMEM = pl.BlockSpec(memory_space=pltpu.VMEM)
IN_SMEM = pl.BlockSpec(memory_space=pltpu.SMEM)


def granted(mib):
    return pltpu.CompilerParams(vmem_limit_bytes=mib * 1024 * 1024)


def attention(c, pieces, keys, values_t, kv_head):
    members, heads, share, width = pieces[0].shape
    tokens = NEAR * members * share
    positions = keys.shape[1]
    per_class = heads // 2
    rows_out = per_class * (width // 2) + 4 * per_class
    return pl.pallas_call(
        functools.partial(attention_kernel, kv_head=kv_head, chunk=512),
        in_specs=[IN_SMEM] + [IN_VMEM] * 6,
        out_specs=IN_VMEM,
        out_shape=jax.ShapeDtypeStruct((NEAR, rows_out, tokens), BF16),
        scratch_shapes=[
            pltpu.VMEM((tokens, width), F32),
            pltpu.VMEM((width + 16, positions), BF16),
            pltpu.VMEM((2, 4 * per_class, tokens), F32),
            pltpu.VMEM((positions, tokens), F32),
            pltpu.VMEM((positions, tokens), F32),
            pltpu.VMEM((8, tokens), F32),
            pltpu.VMEM((8, tokens), F32),
        ],
        compiler_params=granted(20),
        cost_estimate=pl.CostEstimate(
            flops=4 * heads * tokens * positions * width,
            transcendentals=heads * tokens * positions,
            bytes_accessed=4 * positions * width + 4 * tokens * heads * width,
        ),
        name="attention",
    )(c, *pieces, keys, values_t)


def near_combine_kernel(*refs):
    out_ref = refs[-1]
    count, rows, tokens = out_ref.shape
    half = rows - 8
    place = lax.broadcasted_iota(jnp.int32, (8, tokens), 0)
    sets = (len(refs) - 1) // NEAR
    each = count // sets
    for g in range(sets):
        sources = refs[g * NEAR : (g + 1) * NEAR]
        stats = [m[each * half :, :].astype(F32) for m in sources]
        peak = stats[0][:each]
        for s in stats[1:]:
            peak = jnp.maximum(peak, s[:each])
        factors = [jnp.exp2(s[:each] - peak) for s in stats]
        total = sum(f * (s[each : 2 * each] + s[2 * each : 3 * each]) for f, s in zip(factors, stats))
        total_hi = total.astype(BF16).astype(F32)
        total_lo = total - total_hi
        for i in range(each):
            acc = sum(
                f[i : i + 1] * m[i * half : (i + 1) * half, :].astype(F32)
                for f, m in zip(factors, sources)
            )
            out_ref[g * each + i, :half, :] = acc.astype(BF16)
            tail = jnp.where(
                place == 0,
                peak[i : i + 1],
                jnp.where(
                    place == 1, total_hi[i : i + 1], jnp.where(place == 2, total_lo[i : i + 1], 0.0)
                ),
            )
            out_ref[g * each + i, half:, :] = tail.astype(BF16)


def near_combine(sources, count, half):
    tokens = sources[0].shape[1]
    return pl.pallas_call(
        near_combine_kernel,
        in_specs=[IN_VMEM] * len(sources),
        out_specs=IN_VMEM,
        out_shape=jax.ShapeDtypeStruct((count, half + 8, tokens), BF16),
        compiler_params=granted(12),
        name="near_combine",
    )(*sources)


def project_kernel(where_ref, f_ref, w_ref, own_ref, other_ref):
    members, rows, tokens = f_ref.shape
    half = rows - 8
    c, h = where_ref[0], where_ref[1]
    peaks = [f_ref[i, half:, :].astype(F32) for i in range(members)]
    top = peaks[0][0:1]
    for p in peaks[1:]:
        top = jnp.maximum(top, p[0:1])
    total = jnp.zeros((1, tokens), F32)
    acc = jnp.zeros((half, tokens), F32)
    for i in range(members):
        factor = jnp.exp2(peaks[i][0:1] - top)
        total = total + factor * (peaks[i][1:2] + peaks[i][2:3])
        acc = acc + factor * f_ref[i, :half, :].astype(F32)
    attended = (acc / total).astype(BF16)
    share = tokens // (NEAR * members)
    mine = share // 2
    source = lax.broadcasted_iota(jnp.int32, (tokens, tokens), 0)
    target = lax.broadcasted_iota(jnp.int32, (1, tokens), 1)
    side = target // (tokens // 2)
    place = (target // (members * mine)) % NEAR
    offset = sum(jnp.where(place == i, o, 0) for i, o in enumerate(START_ORDER, 1))
    member = (target // mine) % members
    sample = target % mine
    core = (h + side) % 2
    wanted = ((c + offset) % NEAR) * (members * share) + member * share + core * mine + sample
    order = jnp.where(source == wanted, 1.0, 0.0).astype(BF16)
    ordered = contract(attended, order, 1, 0).astype(BF16)
    projected = contract(ordered, w_ref[...], 0, 0)
    own_ref[...] = projected[: tokens // 2].astype(BF16)
    other_ref[...] = projected[tokens // 2 :].astype(BF16)


def project(where, arrived, weight):
    tokens = arrived.shape[2]
    model = weight.shape[1]
    return pl.pallas_call(
        project_kernel,
        in_specs=[IN_SMEM, IN_VMEM, IN_VMEM],
        out_specs=(IN_VMEM, IN_VMEM),
        out_shape=(
            jax.ShapeDtypeStruct((tokens // 2, model), BF16),
            jax.ShapeDtypeStruct((tokens // 2, model), BF16),
        ),
        compiler_params=granted(12),
        name="project",
    )(where, arrived, weight)


def experts_kernel(
    e_ref, near_ref, far_ref, g_hbm, u_hbm, d_hbm, own_ref, other_ref, gs, us, ds, xs, hs, sems, *, block, out_block
):
    side, wide = near_ref.shape
    _, model, ffn = g_hbm.shape
    first = [pl.ds(i, block) for i in range(0, ffn, block)]
    second = [pl.ds(i, out_block) for i in range(0, model, out_block)]
    gates = [pltpu.make_async_copy(g_hbm.at[0, :, b], gs.at[:, b], sems.at[0, i]) for i, b in enumerate(first)]
    ups = [pltpu.make_async_copy(u_hbm.at[0, :, b], us.at[:, b], sems.at[1, i]) for i, b in enumerate(first)]
    downs = [pltpu.make_async_copy(d_hbm.at[0, :, b], ds.at[:, b], sems.at[2, i]) for i, b in enumerate(second)]
    for g, u in zip(gates, ups):
        g.start()
        u.start()
    for d in downs:
        d.start()
    xs[:side] = near_ref[:, :model]
    xs[side:] = far_ref[:, :model]
    lane = lax.broadcasted_iota(jnp.int32, (1, wide - model), 1)
    pick = jnp.where(lane % ((wide - model) // 2) == e_ref[0], 1.0, 0.0)
    factors = [
        jnp.sum(r[:, model:].astype(F32) * pick, axis=1, keepdims=True) for r in (near_ref, far_ref)
    ]
    for b, g, u in zip(first, gates, ups):
        g.wait()
        u.wait()
        gate = contract(xs[...], gs[:, b], 1, 0)
        up = contract(xs[...], us[:, b], 1, 0)
        hs[:, b] = (gate / (1.0 + jnp.exp(-gate)) * up).astype(BF16)
    for b, d in zip(second, downs):
        d.wait()
        part = contract(hs[...], ds[:, b], 1, 0)
        own_ref[:, b] = (part[:side] * factors[0]).astype(BF16)
        other_ref[:, b] = (part[side:] * factors[1]).astype(BF16)


def run_expert(expert, near, far, w_gate, w_up, w_down, block=256, out_block=1024, mib=50):
    side, wide = near.shape
    _, model, ffn = w_gate.shape
    in_hbm = pl.BlockSpec(memory_space=pltpu.HBM)
    shape = jax.ShapeDtypeStruct((side, model), BF16)
    return pl.pallas_call(
        functools.partial(experts_kernel, block=block, out_block=out_block),
        in_specs=[IN_SMEM, IN_VMEM, IN_VMEM, in_hbm, in_hbm, in_hbm],
        out_specs=(IN_VMEM, IN_VMEM),
        out_shape=(shape, shape),
        scratch_shapes=[
            pltpu.VMEM((model, ffn), BF16),
            pltpu.VMEM((model, ffn), BF16),
            pltpu.VMEM((ffn, model), BF16),
            pltpu.VMEM((2 * side, model), BF16),
            pltpu.VMEM((2 * side, ffn), BF16),
            pltpu.SemaphoreType.DMA((3, max(ffn // block, model // out_block))),
        ],
        compiler_params=granted(mib),
        name="experts",
    )(expert, near, far, w_gate, w_up, w_down)


def rows_to_owner(own, other):
    members = lax.axis_size("ctx") // NEAR
    chip = (own.astype(F32) + to_partner(other).astype(F32)).astype(BF16)
    chip = chip.reshape(NEAR, chip.shape[0] // NEAR, chip.shape[1])
    arrived = [near_send(chip[i], o) for i, o in enumerate(START_ORDER, 1)]
    near = (chip[0].astype(F32) + sum(a.astype(F32) for a in arrived)).astype(BF16)
    far = far_exchange(near.reshape(members, near.shape[0] // members, near.shape[1]))
    return far.astype(F32).sum(axis=0)


def on_device(
    queries,
    prefix_keys,
    prefix_values,
    out_weight,
    residual_in,
    expert_ids,
    gate_weights,
    w_gate,
    w_up,
    w_down,
):
    members = lax.axis_size("ctx") // NEAR
    c = lax.rem(lax.axis_index("ctx"), NEAR).astype(jnp.int32)
    h = lax.axis_index("hd").astype(jnp.int32)
    rows_here, model = residual_in.shape
    experts = lax.axis_size("ctx") * lax.axis_size("hd")

    keys = prefix_keys.transpose(1, 0, 2)
    values_t = prefix_values.transpose(1, 2, 0)
    first = far_copies(queries.transpose(1, 0, 2))
    first, keys, values_t = lax.optimization_barrier((first, keys, values_t))
    heads, width = queries.shape[1:]
    kv_heads = keys.shape[0]
    pieces = [[part] + near_fetches(part) for part in jnp.split(first, kv_heads, axis=1)]
    sources = []
    for kv_head in range(kv_heads):
        partial = attention(c[None], pieces[kv_head], keys, values_t, kv_head)
        sources += [partial[0]] + [near_send(partial[o], o) for o in START_ORDER]
    message = near_combine(sources, heads // 2, width // 2)
    own, other = project(jnp.stack([c, h]), far_exchange(message), out_weight)
    projected = rows_to_owner(own, other)

    stream = residual_in.astype(F32) + projected
    normed = stream * lax.rsqrt(jnp.mean(stream * stream, axis=-1, keepdims=True) + 1e-06)
    named = expert_ids[:, :, None] == jnp.arange(experts, dtype=jnp.int32)[None, None, :]
    coefficient = jnp.sum(jnp.where(named, gate_weights[:, :, None], 0.0), axis=1)
    coefficient_hi = lax.reduce_precision(coefficient, 8, 7)
    message = jnp.concatenate(
        [normed, coefficient_hi, coefficient - coefficient_hi], axis=1
    ).astype(BF16)
    first = far_copies(message).reshape(members * rows_here, model + 2 * experts)
    near = jnp.concatenate([first] + near_fetches(first), axis=0)
    expert = lax.axis_index("ctx").astype(jnp.int32) * lax.axis_size("hd") + h
    own, other = run_expert(expert[None], near, to_partner(near), w_gate, w_up, w_down)
    mixture = rows_to_owner(own, other)
    return (stream + mixture).astype(BF16)


def solution(mesh):
    placed = (
        P(("grp", "ctx"), "hd", None),
        P(("grp", "ctx"), "hd", None),
        P(("grp", "ctx"), "hd", None),
        P(("hd", "ctx"), None),
        P(("grp", "ctx", "hd"), None),
        P(("grp", "ctx", "hd"), None),
        P(("grp", "ctx", "hd"), None),
        P(("ctx", "hd"), None, None),
        P(("ctx", "hd"), None, None),
        P(("ctx", "hd"), None, None),
    )
    return jax.shard_map(
        on_device,
        mesh=mesh,
        in_specs=placed,
        out_specs=P(("grp", "ctx", "hd"), None),
        check_vma=False,
    )
```
